128 devices in a mesh: grp: 2 (over z_lo), seq: 32 (over y, x, core), tp: 2 (over z_hi).
Axes of the slice: x: 4, y: 4, z: 4 (z_hi: 2, z_lo: 2; z = z_hi * 2 + z_lo), core: 2. Of those that a mesh axis runs over, the one named last changes fastest.
Arguments:
- latents: bfloat16 [2, 64, 8192], P('grp', None, 'seq'), may hold values from -6 to 6
- patch_weight: bfloat16 [128, 5120], replicated, may hold values from -0.5 to 0.5
- patch_bias: float32 [5120], replicated, may hold values from -3 to 3
- modulation: float32 [3, 5120], replicated, may hold values from -3 to 3
- qkv_weight: bfloat16 [5120, 3, 4096], P(None, None, 'seq'), may hold values from -0.078125 to 0.078125
- norm_gain: float32 [2, 4096], P(None, 'seq'), may hold values from 0.5 to 16
- out_weight: bfloat16 [4096, 5120], P('seq', ('grp', 'tp')), may hold values from -0.5 to 0.5
- token_order: int32 [8192], replicated, may hold values from 0 to 8191, each once
- window_start: int32 [1], replicated, may hold values from 0 to 4096
Outputs:
- attended: bfloat16 [4096, 5120], P('seq', ('grp', 'tp'))
The draws below stay inside these ranges and needn't reach their ends.
Inputs may be any that keep to these rules, and one draw needn't show every extreme that they name: Position j of the target layout holds frame-major token token_order[j]; every token stands once. The window covers target positions window_start[0] to window_start[0] + 4095.
All inputs are finite; a program needn't handle non-finite values.
Results may differ from the reference program's by a relative error of at most 0.018.
The reference program's roundings to bfloat16 on the way (of `stacked`, `normed`, `values`, `probs_low` and `attention`) count: a program that leaves them out, or rounds other values in their place, can miss the bound.
Values may be sent and summed in bfloat16 or wider, within the bound.
A program may use at most 128 MiB of HBM per device.

```python
import math
import jax
import jax.numpy as jnp
from jax import lax

D = 5120
HD = 128
CH = 64
HEADS = 32
TOKENS = 8192
QWIN = 4096


def draw_norm_gain(key, part):
    total_width = HEADS * HD
    base = jnp.exp(jax.random.uniform(key, (2, total_width), jnp.float32, math.log(0.5), math.log(3.0)))
    return base


def level_of(key, extent, shards, least, high):
    gain = 1.0
    for dim, parts in shards:
        draws = jax.random.uniform(jax.random.fold_in(jax.random.fold_in(key, 6), dim), (parts,), jnp.float32, least / len(shards), high / len(shards))
        gain = gain * jnp.repeat(jnp.exp(draws), extent[dim] // parts).reshape((-1,) + (1,) * (len(extent) - 1 - dim))
    return gain


def bell_draw(rng, extent, scale, bound, split=(), kind=jnp.bfloat16):
    factor_of = level_of(rng, extent, split, -0.22, 0.18) if split else 1.0
    drawn = jax.random.normal(rng, extent, jnp.float32) * scale * factor_of
    return jnp.minimum(jnp.maximum(drawn, -bound), bound).astype(kind)


def setup_inputs(seed: int = 0) -> dict:
    splits = jax.random.split(jax.random.key(seed), 10)
    latents = bell_draw(splits[0], (2, CH, TOKENS), 1.0, 6.0, ((0, 2), (2, 32)))
    patch_weight = bell_draw(splits[1], (2 * CH, D), (2 * CH) ** -0.5, 0.5)
    patch_bias = bell_draw(splits[2], (D,), 0.5, 3.0, (), jnp.float32)
    modulation = bell_draw(splits[3], (3, D), 0.5, 3.0, (), jnp.float32)
    qkv_weight = bell_draw(splits[4], (D, 3, HEADS * HD), D ** -0.5, 0.078125, ((2, 32),))
    norm_gain = draw_norm_gain(jax.random.fold_in(splits[9], 71), 0)
    out_weight = bell_draw(splits[6], (HEADS * HD, D), HD ** -0.5, 0.5, ((0, 32), (1, 4)))
    token_order = jax.random.permutation(splits[7], TOKENS).astype(jnp.int32)
    window_start = jax.random.randint(splits[8], (1,), 0, TOKENS - QWIN + 1).astype(jnp.int32)
    return {"latents": latents, "patch_weight": patch_weight, "patch_bias": patch_bias, "modulation": modulation, "qkv_weight": qkv_weight, "norm_gain": norm_gain, "out_weight": out_weight, "token_order": token_order, "window_start": window_start}


norm_eps = 0.1

def reference(latents, patch_weight, patch_bias, modulation, qkv_weight, norm_gain, out_weight, token_order, window_start):
    stacked = jnp.concatenate([latents[0].T, latents[1].T], axis=1)
    embedded = jnp.dot(stacked, patch_weight, preferred_element_type=jnp.float32) + patch_bias
    centre = embedded - lax.optimization_barrier(jnp.mean(embedded, axis=1, keepdims=True))
    spread = lax.optimization_barrier(jnp.mean(centre * centre, axis=1, keepdims=True))
    normed = (centre * lax.rsqrt(spread + norm_eps) * (1.0 + modulation[1]) + modulation[0]).astype(jnp.bfloat16)
    window_rows = lax.dynamic_slice_in_dim(token_order, window_start[0], QWIN)
    picked = jnp.take(normed, window_rows, axis=0)
    query_raw = jnp.dot(picked, qkv_weight[:, 0, :], preferred_element_type=jnp.float32)
    key_raw = jnp.dot(normed, qkv_weight[:, 1, :], preferred_element_type=jnp.float32)
    values = jnp.dot(normed, qkv_weight[:, 2, :], preferred_element_type=jnp.float32).astype(jnp.bfloat16)
    query_mean = lax.optimization_barrier(jnp.mean(query_raw * query_raw, axis=1, keepdims=True))
    key_mean = lax.optimization_barrier(jnp.mean(key_raw * key_raw, axis=1, keepdims=True))
    queries = (query_raw * lax.rsqrt(query_mean + norm_eps) * norm_gain[0]).astype(jnp.bfloat16)
    keys = (key_raw * lax.rsqrt(key_mean + norm_eps) * norm_gain[1]).astype(jnp.bfloat16)
    head_queries = queries.reshape(QWIN, HEADS, HD).transpose(1, 0, 2)
    head_keys = keys.reshape(TOKENS, HEADS, HD).transpose(1, 0, 2)
    head_values = values.reshape(TOKENS, HEADS, HD).transpose(1, 0, 2)

    def attend(operands):
        query_head, key_head, value_head = operands
        scores = jnp.dot(query_head, key_head.T, preferred_element_type=jnp.float32) * HD ** (-0.5)
        probs = jnp.exp(scores - lax.optimization_barrier(jnp.max(scores, axis=1, keepdims=True)))
        probs_low = probs.astype(jnp.bfloat16)
        summed = jnp.dot(probs_low, value_head, preferred_element_type=jnp.float32)
        return (summed / lax.optimization_barrier(jnp.sum(probs, axis=1, keepdims=True))).astype(jnp.bfloat16)
    attention = lax.map(attend, (head_queries, head_keys, head_values))
    attention = attention.transpose(1, 0, 2).reshape(QWIN, HEADS * HD)
    mixed = jnp.dot(attention, out_weight, preferred_element_type=jnp.float32)
    return (mixed * modulation[2]).astype(jnp.bfloat16)
```

```python
import jax
import jax.numpy as jnp
from jax import lax
from jax.sharding import PartitionSpec as P

EPS = 0.1
HI = lax.Precision.HIGHEST


def split_dot(a, w):
    high = a.astype(jnp.bfloat16)
    low = (a - high.astype(jnp.float32)).astype(jnp.bfloat16)
    both = jnp.dot(jnp.concatenate([high, low], 0), w, preferred_element_type=jnp.float32)
    return both[: a.shape[0]] + both[a.shape[0] :]


def per_device(
    latents, patch_weight, patch_bias, modulation, qkv_weight, norm_gain, out_weight, token_order, window_start
):
    width, _, hd = qkv_weight.shape
    n_seq = lax.axis_size("seq")
    quarter = lax.axis_index("grp") * lax.axis_size("tp") + lax.axis_index("tp")
    groups = lax.axis_size("grp") * lax.axis_size("tp")
    pw = patch_weight.astype(jnp.float32)
    pwc = pw - jnp.mean(pw, axis=1, keepdims=True)
    bc = (patch_bias - jnp.mean(patch_bias))[None]
    centred = jnp.concatenate([pwc, bc], 0)
    gram = jnp.dot(centred, centred.T, precision=HI) / width
    scale = (1.0 + modulation[1])[None]
    folded = jnp.concatenate([centred * scale, modulation[0][None]], 0)
    planes = qkv_weight.transpose(1, 0, 2)
    mq, mk, mv = (split_dot(folded, planes[i]) for i in range(3))
    ext = mq.shape[0]
    pad = -(2 * ext * ext) % (n_seq * 128)
    mine = jnp.stack([jnp.dot(mq, mq.T, precision=HI), jnp.dot(mk, mk.T, precision=HI)])
    mine = jnp.pad(mine.reshape(-1), (0, pad)).reshape(n_seq, -1)
    parts = lax.all_to_all(mine, "seq", split_axis=0, concat_axis=0, tiled=True)
    total = lax.all_gather(jnp.sum(parts, axis=0), "seq", axis=0, tiled=True)
    norms = (total[: 2 * ext * ext] / (hd * n_seq)).reshape(2, ext, ext)
    partner = lax.ppermute(latents, "grp", [(0, 1), (1, 0)])
    first = lax.axis_index("grp") == 0
    paired = jnp.where(
        first, jnp.concatenate([latents, partner], 0), jnp.concatenate([partner, latents], 0)
    ).reshape(-1, latents.shape[2])
    rows = lax.all_gather(paired.T, "seq", axis=0, tiled=True)
    window = lax.dynamic_slice_in_dim(token_order, window_start[0], 128 * n_seq)
    sub = 128 // groups
    picked = lax.dynamic_slice_in_dim(window.reshape(n_seq, groups, sub), quarter, 1, 1).reshape(-1)
    qrows = jnp.take(rows, picked, axis=0)

    def extended(x):
        x = jnp.concatenate([x.astype(jnp.float32), jnp.ones((x.shape[0], 1), jnp.float32)], 1)
        spread = jnp.sum(jnp.dot(x, gram, precision=HI) * x, axis=1, keepdims=True)
        x = x * lax.rsqrt(spread + EPS)
        return jnp.concatenate([x, jnp.ones((x.shape[0], 1), jnp.float32)], 1)

    def normalized(x, weight, norm, gain):
        mean = jnp.sum(jnp.dot(x, norm, precision=HI) * x, axis=1, keepdims=True)
        return (jnp.dot(x, weight, precision=HI) * lax.rsqrt(mean + EPS) * gain).astype(jnp.bfloat16)

    kx = extended(rows)
    keys = normalized(kx, mk, norms[1], norm_gain[1])
    values = jnp.dot(kx, mv, precision=HI).astype(jnp.bfloat16)
    queries = normalized(extended(qrows), mq, norms[0], norm_gain[0])

    def attend(block):
        scores = jnp.dot(block, keys.T, preferred_element_type=jnp.float32) * hd ** (-0.5)
        probs = jnp.exp(scores - jnp.max(scores, axis=1, keepdims=True))
        summed = jnp.dot(probs.astype(jnp.bfloat16), values, preferred_element_type=jnp.float32)
        return (summed / jnp.sum(probs, axis=1, keepdims=True)).astype(jnp.bfloat16)

    attention = lax.map(attend, queries.reshape(-1, 128, hd)).reshape(n_seq, sub, hd)
    regrouped = lax.all_to_all(attention, "seq", split_axis=0, concat_axis=0, tiled=True)
    regrouped = regrouped.transpose(1, 0, 2).reshape(sub, n_seq * hd)
    regrouped = lax.all_gather(regrouped, ("grp", "tp"), axis=0, tiled=True)
    cols = out_weight.shape[1]
    gate = lax.dynamic_slice_in_dim(modulation[2], quarter * cols, cols)
    mixed = jnp.dot(
        regrouped, lax.all_gather(out_weight, "seq", axis=0, tiled=True), preferred_element_type=jnp.float32
    )
    return (mixed * gate).astype(jnp.bfloat16)


def solution(mesh):
    in_specs = (
        P("grp", None, "seq"), P(), P(), P(), P(None, None, "seq"), P(None, "seq"), P("seq", ("grp", "tp")), P(), P(),
    )
    return jax.shard_map(
        per_device, mesh=mesh, in_specs=in_specs, out_specs=P("seq", ("grp", "tp")), check_vma=False
    )
```
